32 devices in a mesh: rows: 8 (over z, y), grp: 4 (over x, core).
Axes of the slice: x: 2, y: 2, z: 4, core: 2. Of those that a mesh axis runs over, the one named last changes fastest.
Arguments:
- activations: bfloat16 [3072, 2048], P(('rows', 'grp')), may hold values from 0 to 1
- weight_tiles: bfloat16 [3, 512, 2, 128, 128], P(None, ('rows', 'grp')), may hold values from -0.75 to 0.75
- tile_index: int32 [3, 512, 1], replicated, may hold values from 0 to 511, as said below
- bias_terms: float32 [3, 65536], replicated, may hold values from -0.3 to 0.3
- demand: int32 [32, 16], P(('rows', 'grp')), may hold values from 0 to 511, as said below
Outputs:
- final_acts: bfloat16 [3072, 2048], P(('rows', 'grp'))
The draws below stay inside these ranges and needn't reach their ends.
Inputs may be any that keep to these rules, and one draw needn't show every extreme that they name: Each row of demand lists 16 distinct blocks made of whole groups [g * 4, (g + 1) * 4); every range [r * 64, (r + 1) * 64) holds either none of them or exactly one group of 4. tile_index[l, b, k] is a block of b's own group [(b // 4) * 4, (b // 4 + 1) * 4), never b itself.
All inputs are finite; a program needn't handle non-finite values.
Results may differ from the reference program's by a relative error of at most 0.0057.
Values may be sent and summed in bfloat16 or wider, within the bound.
A program may use at most 128 MiB of HBM per device.

```python
import jax
import jax.numpy as jnp
from jax import lax

NEURONS = 65536
TILE = 128
NB = 512
LAYERS = 3
K_OFF = 1
CAP = 4
BPR = 64
LIVE = 16
R_DEV = 96
TOTAL_ROWS = 3072
N_ROWS = 8
DEVICES = 32


def draw_tile_index(key, part):
    block_count = NEURONS // TILE
    offsets = jax.random.randint(jax.random.fold_in(key, 11), (LAYERS, block_count, K_OFF), 1, CAP).astype(jnp.int32)
    blocks = jnp.arange(block_count, dtype=jnp.int32)[None, :, None]
    members = (blocks % CAP + offsets) % CAP
    return (blocks // CAP * CAP + members).astype(jnp.int32)


def draw_demand(key, part):

    def one_device(dev_key):
        key_range, key_group, key_order = jax.random.split(dev_key, 3)
        ranges = jax.random.permutation(key_range, N_ROWS)[:N_ROWS // 2].astype(jnp.int32)
        groups = jax.random.randint(key_group, (N_ROWS // 2,), 0, BPR // CAP).astype(jnp.int32)
        starts = ranges * BPR + groups * CAP
        blocks = (starts[:, None] + jnp.arange(CAP, dtype=jnp.int32)[None, :]).reshape(-1)
        return jax.random.permutation(key_order, blocks).astype(jnp.int32)
    return jax.vmap(one_device)(jax.random.split(jax.random.fold_in(key, 23), DEVICES))


def shard_levels(rng, extent, shards, smallest, high):
    def one(axis_at, shards_of):
        heights = jax.random.uniform(jax.random.fold_in(jax.random.fold_in(rng, 6), axis_at), (shards_of,), jnp.float32, smallest / len(shards), high / len(shards))
        return jnp.repeat(jnp.exp(heights), extent[axis_at] // shards_of).reshape((-1,) + (1,) * (len(extent) - axis_at - 1))

    factor_of = one(*shards[0])
    for cut in shards[1:]:
        factor_of = factor_of * one(*cut)
    return factor_of


def bell_draw(rng, dims, scale, bound, shards=(), kind=jnp.bfloat16):
    gain = shard_levels(rng, dims, shards, -0.22, 0.18) if shards else 1.0
    array = jax.random.normal(rng, dims, jnp.float32) * scale * gain
    return jnp.minimum(jnp.maximum(array, -bound), bound).astype(kind)


def setup_inputs(seed: int = 0) -> dict:
    key_of = jax.random.split(jax.random.key(seed), 6)
    activations = jnp.clip(1.0 * jax.random.uniform(key_of[0], (TOTAL_ROWS, LIVE * TILE), jnp.float32) ** shard_levels(key_of[0], (TOTAL_ROWS, LIVE * TILE), ((0, 32),), -0.2, 0.2), 0.0, 1.0).astype(jnp.bfloat16)
    weight_tiles = bell_draw(key_of[1], (LAYERS, NB, 1 + K_OFF, TILE, TILE), (TILE // 2) ** -0.5, 0.75, ((1, 32),))
    tile_index = draw_tile_index(jax.random.fold_in(key_of[5], 71), 0)
    bias_terms = jnp.clip(jax.random.uniform(key_of[3], (LAYERS, NEURONS), jnp.float32, -0.3, 0.3), -0.3, 0.3)
    demand = draw_demand(jax.random.fold_in(key_of[5], 71), 0)
    return {"activations": activations, "weight_tiles": weight_tiles, "tile_index": tile_index, "bias_terms": bias_terms, "demand": demand}


def reference(activations, weight_tiles, tile_index, bias_terms, demand):
    block_count = NEURONS // TILE
    acts = activations.reshape(DEVICES, R_DEV, LIVE, TILE)
    bias_blocks = bias_terms.reshape(LAYERS, block_count, TILE)

    def one_device(inputs):
        current, live_blocks = inputs
        for layer_num in range(LAYERS):
            weights = weight_tiles[layer_num][live_blocks].astype(jnp.float32)
            off_blocks = tile_index[layer_num][live_blocks]
            matches = (off_blocks[:, :, None] == live_blocks[None, None, :]).astype(jnp.float32)
            chosen = jnp.einsum('ikp,rpt->rikt', matches, current.astype(jnp.float32))
            diag_part = jnp.einsum('rit,itu->riu', current.astype(jnp.float32), weights[:, 0])
            off_part = jnp.einsum('rikt,iktu->riu', chosen, weights[:, 1:])
            pre_act = diag_part + off_part + bias_blocks[layer_num][live_blocks][None]
            current = jax.nn.relu(pre_act).astype(jnp.bfloat16)
        return current

    result = lax.map(one_device, (acts, demand))
    return result.reshape(DEVICES * R_DEV, LIVE * TILE)
```

```python
import functools

import jax
import jax.numpy as jnp
from jax import lax
from jax.experimental import pallas as pl
from jax.experimental.pallas import tpu as pltpu
from jax.sharding import PartitionSpec as P

CAP = 4
CORES = 2
PLANES = 2
LAG = 3
MESH = pl.DeviceIdType.MESH


def group_step(state, weights, matches, bias_rows):
    chosen = jnp.einsum(
        "sckp,srpt->srckt", matches, state, preferred_element_type=jnp.float32
    ).astype(jnp.bfloat16)
    diag_part = jnp.einsum(
        "srct,sctu->srcu", state, weights[:, :, 0], preferred_element_type=jnp.float32
    )
    off_part = jnp.einsum(
        "srckt,scktu->srcu", chosen, weights[:, :, 1:], preferred_element_type=jnp.float32
    )
    return jax.nn.relu(diag_part + off_part + bias_rows[:, None]).astype(jnp.bfloat16)


def gathered_shards(activations, weight_tiles, tile_index, bias_terms, demand):
    live_blocks = demand[0]
    live_count = live_blocks.shape[0]
    tile_width = weight_tiles.shape[-1]
    row_count = lax.axis_size("rows")
    per_range = weight_tiles.shape[1] * lax.axis_size("grp")
    owners = live_blocks // per_range
    within = live_blocks % per_range
    range_ids = jnp.arange(row_count, dtype=jnp.int32)
    slot_ids = jnp.arange(CAP, dtype=jnp.int32)
    current = activations.reshape(activations.shape[0], live_count, tile_width)
    bias_blocks = bias_terms.reshape(bias_terms.shape[0], -1, tile_width)
    grouped = lax.all_gather(weight_tiles, "grp", axis=1, tiled=True)
    member = live_blocks % CAP
    placing = (owners[None, None, :] == range_ids[:, None, None]) & (
        member[None, None, :] == slot_ids[None, :, None]
    )
    starts = jnp.sum(placing[:, 0, :].astype(jnp.int32) * (within[None, :] + 1), axis=1) - 1
    outgoing = jnp.einsum(
        "acp,rpt->arct", placing.astype(jnp.bfloat16), current, preferred_element_type=jnp.float32
    ).astype(jnp.bfloat16)
    arrived = lax.all_to_all(outgoing, "rows", split_axis=0, concat_axis=0, tiled=True)
    bases = lax.all_to_all(
        starts.reshape(row_count, 1), "rows", split_axis=0, concat_axis=0, tiled=True
    )[:, 0]
    slot_blocks = jnp.clip(bases, 0)[:, None] + slot_ids[None, :]
    global_blocks = lax.axis_index("rows") * per_range + slot_blocks
    state = arrived
    for layer_num in range(weight_tiles.shape[0]):
        weights = grouped[layer_num][slot_blocks]
        off_member = tile_index[layer_num][global_blocks] % CAP
        matches = (off_member[:, :, :, None] == slot_ids[None, None, None, :]).astype(jnp.bfloat16)
        state = group_step(state, weights, matches, bias_blocks[layer_num][global_blocks])
    returned = lax.all_to_all(state, "rows", split_axis=0, concat_axis=0, tiled=True)
    current = jnp.einsum(
        "acp,arct->rpt", placing.astype(jnp.bfloat16), returned, preferred_element_type=jnp.float32
    ).astype(jnp.bfloat16)
    return current.reshape(current.shape[0], live_count * tile_width)


def fused_kernel(
    n, pos_ref, home_ref, index_ref, meta_ref, act_ref, bias_ref, w_hbm, out_ref,
    w_all, slots, zin, xin, ores, fres, xres, sel, fin, st_own, st_for, meta_in, meta_s,
    w_sems, m_send, m_recv, m_copy, z_send, z_recv, x_send, x_recv,
    b_send, b_recv, f_send, f_recv,
):
    layers, held = w_hbm.shape[0], w_hbm.shape[1]
    tile = w_hbm.shape[-1]
    live = home_ref.shape[1]
    r = lax.axis_index("rows")
    g = lax.axis_index("grp")
    plane, core = g // CORES, g % CORES
    mate = plane * CORES + (CORES - 1 - core)
    cross = (PLANES - 1 - plane) * CORES + core

    def up(k):
        return lax.rem(r + k, n)

    def down(k):
        return lax.rem(r - k + n, n)

    barrier = pltpu.get_barrier_semaphore()
    pl.semaphore_signal(barrier, inc=1, device_id=(r, mate), device_id_type=MESH)

    def greet(k, carry):
        pl.semaphore_signal(barrier, inc=1, device_id=(up(k), g), device_id_type=MESH)
        pl.semaphore_signal(barrier, inc=1, device_id=(up(k), cross), device_id_type=MESH)
        return carry

    lax.fori_loop(1, n, greet, 0)
    pl.semaphore_signal(barrier, inc=1, device_id=(r, cross), device_id_type=MESH)

    w_local = pltpu.make_async_copy(w_hbm, w_all.at[core], w_sems.at[0])
    w_local.start()
    for a in range(n):
        for c in range(CAP):
            slots[a, c] = act_ref[pos_ref[a, c]]
    meta_in[0, r] = meta_ref[r]
    pl.semaphore_wait(barrier, 2 * n)

    def meta_copy(which, slot, row, dev_row, dev_grp):
        return pltpu.make_async_remote_copy(
            src_ref=meta_ref.at[row], dst_ref=meta_in.at[which, slot],
            send_sem=m_send.at[which, row], recv_sem=m_recv.at[which, slot],
            device_id=(dev_row, dev_grp), device_id_type=MESH,
        )

    def z_copy(row, slot):
        return pltpu.make_async_remote_copy(
            src_ref=slots.at[row], dst_ref=zin.at[slot],
            send_sem=z_send.at[row], recv_sem=z_recv.at[slot],
            device_id=(row, g), device_id_type=MESH,
        )

    def x_copy(src, slot):
        return pltpu.make_async_remote_copy(
            src_ref=src.at[slot], dst_ref=xin.at[slot],
            send_sem=x_send.at[slot], recv_sem=x_recv.at[slot],
            device_id=(r, cross), device_id_type=MESH,
        )

    def b_copy(slot):
        return pltpu.make_async_remote_copy(
            src_ref=fres.at[slot], dst_ref=xres.at[slot],
            send_sem=b_send.at[slot], recv_sem=b_recv.at[slot],
            device_id=(r, cross), device_id_type=MESH,
        )

    def f_copy(row, slot):
        return pltpu.make_async_remote_copy(
            src_ref=sel.at[row], dst_ref=fin.at[slot],
            send_sem=f_send.at[row], recv_sem=f_recv.at[slot],
            device_id=(row, g), device_id_type=MESH,
        )

    w_remote = pltpu.make_async_remote_copy(
        src_ref=w_hbm, dst_ref=w_all.at[core],
        send_sem=w_sems.at[1], recv_sem=w_sems.at[2],
        device_id=(r, mate), device_id_type=MESH,
    )
    w_arrives = pltpu.make_async_remote_copy(
        src_ref=w_hbm, dst_ref=w_all.at[CORES - 1 - core],
        send_sem=w_sems.at[1], recv_sem=w_sems.at[2],
        device_id=(r, mate), device_id_type=MESH,
    )

    def send_meta(k, carry):
        row = up(k)
        meta_copy(0, r, row, row, g).start()
        meta_copy(1, r, row, row, cross).start()
        return carry

    x_copy(slots, r).start()
    meta_copy(1, r, r, r, cross).start()
    lax.fori_loop(1, n, send_meta, 0)

    def send_rows(k, carry):
        z_copy(up(k), r).start()
        return carry

    lax.fori_loop(1, n, send_rows, 0)
    w_remote.start()

    def forward(k):
        slot = down(k)
        z_copy(r, slot).wait_recv()
        x_copy(zin, slot).start()

    for k in range(1, min(LAG, n)):
        forward(k)
    meta_copy(1, r, r, r, cross).wait_recv()

    def take_meta(k, carry):
        meta_copy(0, down(k), r, r, g).wait_recv()
        meta_copy(1, down(k), r, r, cross).wait_recv()
        return carry

    lax.fori_loop(1, n, take_meta, 0)
    to_smem = pltpu.make_async_copy(meta_in, meta_s, m_copy)
    to_smem.start()
    to_smem.wait()
    w_local.wait()
    w_arrives.wait_recv()

    def compute(jobs):
        for load, slot, _, state, _ in jobs:
            for j in range(CAP):
                state[0, j] = load[slot, j]
        for layer in range(layers):
            for _, slot, store, state, which in jobs:
                half = meta_s[which, slot, 0, 0]
                local = meta_s[which, slot, 0, 1]
                inner = meta_s[which, slot, 0, 2]
                for j in range(CAP):
                    other = index_ref[layer, inner + j]
                    pair = (state[layer % 2, j], state[layer % 2, other])
                    pre = jnp.dot(
                        jnp.concatenate(pair, axis=1), w_all[half, layer, local + j],
                        preferred_element_type=jnp.float32,
                    ) + bias_ref[layer, inner + j]
                    value = jnp.maximum(pre, 0.0).astype(jnp.bfloat16)
                    if layer == layers - 1:
                        store[slot, j] = value
                    else:
                        state[(layer + 1) % 2, j] = value

    def step(k, own_buf):
        slot = down(k)
        x_copy(zin, slot).wait_recv()
        compute((
            (xin, slot, fres, st_for, 1),
            (own_buf, slot, ores, st_own, 0),
        ))
        b_copy(slot).start()

    def choose(slot):
        b_copy(slot).wait_recv()
        mine = (meta_s[0, slot, 0, 3] == plane).astype(jnp.float32)
        for j in range(CAP):
            sel[slot, j] = (
                ores[slot, j].astype(jnp.float32) * mine
                + xres[slot, j].astype(jnp.float32) * (1.0 - mine)
            ).astype(jnp.bfloat16)

    if LAG < n:
        forward(LAG)
    step(0, slots)

    def early(k, carry):
        forward(k + LAG)
        step(k, zin)
        return carry

    lax.fori_loop(1, n - LAG, early, 0)
    choose(r)

    def late(k, carry):
        step(k, zin)
        slot = down(k - (n - LAG) + 1)
        choose(slot)
        f_copy(slot, r).start()
        return carry

    lax.fori_loop(n - LAG, n, late, 0)

    def last(k, carry):
        slot = down(k)
        choose(slot)
        f_copy(slot, r).start()
        return carry

    lax.fori_loop(LAG + 1, n, last, 0)

    def take(k, carry):
        f_copy(r, down(k)).wait_recv()
        return carry

    lax.fori_loop(1, n, take, 0)
    fin[r] = sel[r]
    for p in range(live):
        out_ref[:, p * tile:(p + 1) * tile] = fin[home_ref[0, p], home_ref[1, p]]

    def drain(k, carry):
        row = up(k)
        meta_copy(0, r, row, row, g).wait_send()
        meta_copy(1, r, row, row, cross).wait_send()
        z_copy(row, r).wait_send()
        x_copy(zin, row).wait_send()
        b_copy(row).wait_send()
        f_copy(row, r).wait_send()
        return carry

    lax.fori_loop(1, n, drain, 0)
    meta_copy(1, r, r, r, cross).wait_send()
    x_copy(slots, r).wait_send()
    b_copy(r).wait_send()
    w_remote.wait_send()


def fused_shards(activations, weight_tiles, tile_index, bias_terms, demand):
    n = lax.axis_size("rows")
    layers, held, kinds, tile, _ = weight_tiles.shape
    per_range = held * lax.axis_size("grp")
    depth = activations.shape[0]
    blocks = demand[0]
    owners, within, member = blocks // per_range, blocks % per_range, blocks % CAP
    placing = (owners[None, None, :] == jnp.arange(n, dtype=jnp.int32)[:, None, None]) & (
        member[None, None, :] == jnp.arange(CAP, dtype=jnp.int32)[None, :, None]
    )
    places = jnp.arange(blocks.shape[0], dtype=jnp.int32)
    pos = jnp.sum(jnp.where(placing, places, 0), axis=2)
    starts = jnp.sum(jnp.where(placing[:, 0], within, 0), axis=1)
    chip_blocks = held * CORES
    inner = starts % chip_blocks
    facts = jnp.stack([inner // held, inner % held, inner, starts // chip_blocks], axis=1)
    meta = jnp.pad(facts, ((0, 0), (0, 124)))[:, None, :]
    home = jnp.stack([owners, member])
    chip = (lax.axis_index("rows") * PLANES + lax.axis_index("grp") // CORES) * chip_blocks
    others = lax.dynamic_slice_in_dim(tile_index[:, :, 0], chip, chip_blocks, axis=1) % CAP
    bias = lax.dynamic_slice_in_dim(bias_terms, chip * tile, chip_blocks * tile, axis=1)
    bias = bias.reshape(layers, chip_blocks, 1, tile)
    weights = weight_tiles.reshape(layers, held, kinds * tile, tile)
    columns = activations.reshape(depth, blocks.shape[0], tile).transpose(1, 0, 2)
    smem = pl.BlockSpec(memory_space=pltpu.SMEM)
    vmem = pl.BlockSpec(memory_space=pltpu.VMEM)
    slot = pltpu.VMEM((n, CAP, depth, tile), jnp.bfloat16)
    sems = pltpu.SemaphoreType.DMA((n,))
    return pl.pallas_call(
        functools.partial(fused_kernel, n),
        out_shape=jax.ShapeDtypeStruct(activations.shape, jnp.bfloat16),
        in_specs=[smem, smem, smem, vmem, vmem, vmem, pl.BlockSpec(memory_space=pl.ANY)],
        out_specs=vmem,
        scratch_shapes=[
            pltpu.VMEM((CORES, layers, held, kinds * tile, tile), jnp.bfloat16),
            slot, slot, slot, slot, slot, slot, slot, slot,
            pltpu.VMEM((2, CAP, depth, tile), jnp.bfloat16),
            pltpu.VMEM((2, CAP, depth, tile), jnp.bfloat16),
            pltpu.VMEM((2, n, 1, 128), jnp.int32),
            pltpu.SMEM((2, n, 1, 128), jnp.int32),
            pltpu.SemaphoreType.DMA((3,)),
            pltpu.SemaphoreType.DMA((2, n)),
            pltpu.SemaphoreType.DMA((2, n)),
            pltpu.SemaphoreType.DMA,
            sems, sems, sems, sems, sems, sems, sems, sems,
        ],
        compiler_params=pltpu.CompilerParams(
            collective_id=0, has_side_effects=True, vmem_limit_bytes=40 * 1024 * 1024
        ),
    )(pos, home, others, meta, columns, bias, weights)


def solution(mesh):
    def shards(activations, weight_tiles, tile_index, bias_terms, demand):
        whole_groups = weight_tiles.shape[1] % CAP == 0 and weight_tiles.shape[2] == 2
        if whole_groups and mesh.shape["grp"] == PLANES * CORES and mesh.shape["rows"] > 2 * LAG:
            return fused_shards(activations, weight_tiles, tile_index, bias_terms, demand)
        return gathered_shards(activations, weight_tiles, tile_index, bias_terms, demand)

    return jax.shard_map(
        shards,
        mesh=mesh,
        in_specs=(
            P(("rows", "grp"), None),
            P(None, ("rows", "grp"), None, None, None),
            P(),
            P(),
            P(("rows", "grp"), None),
        ),
        out_specs=P(("rows", "grp"), None),
        check_vma=False,
    )
```

```python
import functools

import jax
import jax.numpy as jnp
from jax import lax
from jax.experimental import pallas as pl
from jax.experimental.pallas import tpu as pltpu
from jax.sharding import PartitionSpec as P

CAP = 4
CORES = 2
PLANES = 2
LAG = 3
BACK = 2
MESH = pl.DeviceIdType.MESH


def group_step(state, weights, matches, bias_rows):
    chosen = jnp.einsum(
        "sckp,srpt->srckt", matches, state, preferred_element_type=jnp.float32
    ).astype(jnp.bfloat16)
    diag_part = jnp.einsum(
        "srct,sctu->srcu", state, weights[:, :, 0], preferred_element_type=jnp.float32
    )
    off_part = jnp.einsum(
        "srckt,scktu->srcu", chosen, weights[:, :, 1:], preferred_element_type=jnp.float32
    )
    return jax.nn.relu(diag_part + off_part + bias_rows[:, None]).astype(jnp.bfloat16)


def gathered_shards(activations, weight_tiles, tile_index, bias_terms, demand):
    live_blocks = demand[0]
    live_count = live_blocks.shape[0]
    tile_width = weight_tiles.shape[-1]
    row_count = lax.axis_size("rows")
    per_range = weight_tiles.shape[1] * lax.axis_size("grp")
    owners = live_blocks // per_range
    within = live_blocks % per_range
    range_ids = jnp.arange(row_count, dtype=jnp.int32)
    slot_ids = jnp.arange(CAP, dtype=jnp.int32)
    current = activations.reshape(activations.shape[0], live_count, tile_width)
    bias_blocks = bias_terms.reshape(bias_terms.shape[0], -1, tile_width)
    grouped = lax.all_gather(weight_tiles, "grp", axis=1, tiled=True)
    member = live_blocks % CAP
    placing = (owners[None, None, :] == range_ids[:, None, None]) & (
        member[None, None, :] == slot_ids[None, :, None]
    )
    starts = jnp.sum(placing[:, 0, :].astype(jnp.int32) * (within[None, :] + 1), axis=1) - 1
    outgoing = jnp.einsum(
        "acp,rpt->arct", placing.astype(jnp.bfloat16), current, preferred_element_type=jnp.float32
    ).astype(jnp.bfloat16)
    arrived = lax.all_to_all(outgoing, "rows", split_axis=0, concat_axis=0, tiled=True)
    bases = lax.all_to_all(
        starts.reshape(row_count, 1), "rows", split_axis=0, concat_axis=0, tiled=True
    )[:, 0]
    slot_blocks = jnp.clip(bases, 0)[:, None] + slot_ids[None, :]
    global_blocks = lax.axis_index("rows") * per_range + slot_blocks
    state = arrived
    for layer_num in range(weight_tiles.shape[0]):
        weights = grouped[layer_num][slot_blocks]
        off_member = tile_index[layer_num][global_blocks] % CAP
        matches = (off_member[:, :, :, None] == slot_ids[None, None, None, :]).astype(jnp.bfloat16)
        state = group_step(state, weights, matches, bias_blocks[layer_num][global_blocks])
    returned = lax.all_to_all(state, "rows", split_axis=0, concat_axis=0, tiled=True)
    current = jnp.einsum(
        "acp,arct->rpt", placing.astype(jnp.bfloat16), returned, preferred_element_type=jnp.float32
    ).astype(jnp.bfloat16)
    return current.reshape(current.shape[0], live_count * tile_width)


def fused_kernel(
    n, pos_ref, home_ref, index_ref, meta_ref, act_ref, bias_ref, w_hbm, out_ref,
    w_all, slots, zin, xin, ores, fres, xres, sel, fin, st_own, st_for, meta_in, meta_s,
    w_sems, m_send, m_recv, m_copy, z_send, z_recv, x_send, x_recv,
    b_send, b_recv, f_send, f_recv,
):
    layers, held = w_hbm.shape[0], w_hbm.shape[1]
    tile = w_hbm.shape[-1]
    live = home_ref.shape[1]
    r = lax.axis_index("rows")
    g = lax.axis_index("grp")
    plane, core = g // CORES, g % CORES
    mate = plane * CORES + (CORES - 1 - core)
    cross = (PLANES - 1 - plane) * CORES + core

    def up(k):
        return lax.rem(r + k, n)

    def down(k):
        return lax.rem(r - k + n, n)

    barrier = pltpu.get_barrier_semaphore()
    pl.semaphore_signal(barrier, inc=1, device_id=(r, mate), device_id_type=MESH)

    def greet(k, carry):
        pl.semaphore_signal(barrier, inc=1, device_id=(up(k), g), device_id_type=MESH)
        pl.semaphore_signal(barrier, inc=1, device_id=(up(k), cross), device_id_type=MESH)
        return carry

    lax.fori_loop(1, n, greet, 0)
    pl.semaphore_signal(barrier, inc=1, device_id=(r, cross), device_id_type=MESH)

    w_local = pltpu.make_async_copy(w_hbm, w_all.at[core], w_sems.at[0])
    w_local.start()
    for a in range(n):
        for c in range(CAP):
            slots[a, c] = act_ref[pos_ref[a, c]]
    meta_in[0, r] = meta_ref[r]
    pl.semaphore_wait(barrier, 2 * n)

    def meta_copy(which, slot, row, dev_row, dev_grp):
        return pltpu.make_async_remote_copy(
            src_ref=meta_ref.at[row], dst_ref=meta_in.at[which, slot],
            send_sem=m_send.at[which, row], recv_sem=m_recv.at[which, slot],
            device_id=(dev_row, dev_grp), device_id_type=MESH,
        )

    def z_copy(row, slot):
        return pltpu.make_async_remote_copy(
            src_ref=slots.at[row], dst_ref=zin.at[slot],
            send_sem=z_send.at[row], recv_sem=z_recv.at[slot],
            device_id=(row, g), device_id_type=MESH,
        )

    def x_copy(src, slot):
        return pltpu.make_async_remote_copy(
            src_ref=src.at[slot], dst_ref=xin.at[slot],
            send_sem=x_send.at[slot], recv_sem=x_recv.at[slot],
            device_id=(r, cross), device_id_type=MESH,
        )

    def b_copy(slot):
        return pltpu.make_async_remote_copy(
            src_ref=fres.at[slot], dst_ref=xres.at[slot],
            send_sem=b_send.at[slot], recv_sem=b_recv.at[slot],
            device_id=(r, cross), device_id_type=MESH,
        )

    def f_copy(row, slot):
        return pltpu.make_async_remote_copy(
            src_ref=sel.at[row], dst_ref=fin.at[slot],
            send_sem=f_send.at[row], recv_sem=f_recv.at[slot],
            device_id=(row, g), device_id_type=MESH,
        )

    w_remote = pltpu.make_async_remote_copy(
        src_ref=w_hbm, dst_ref=w_all.at[core],
        send_sem=w_sems.at[1], recv_sem=w_sems.at[2],
        device_id=(r, mate), device_id_type=MESH,
    )
    w_arrives = pltpu.make_async_remote_copy(
        src_ref=w_hbm, dst_ref=w_all.at[CORES - 1 - core],
        send_sem=w_sems.at[1], recv_sem=w_sems.at[2],
        device_id=(r, mate), device_id_type=MESH,
    )

    def send_meta(k, carry):
        row = up(k)
        meta_copy(0, r, row, row, g).start()
        meta_copy(1, r, row, row, cross).start()
        return carry

    x_copy(slots, r).start()
    meta_copy(1, r, r, r, cross).start()
    lax.fori_loop(1, n, send_meta, 0)

    def send_rows(k, carry):
        z_copy(up(k), r).start()
        return carry

    lax.fori_loop(1, n, send_rows, 0)
    w_remote.start()

    def forward(k):
        slot = down(k)
        z_copy(r, slot).wait_recv()
        x_copy(zin, slot).start()

    for k in range(1, min(LAG, n)):
        forward(k)
    meta_copy(1, r, r, r, cross).wait_recv()

    def take_meta(k, carry):
        meta_copy(0, down(k), r, r, g).wait_recv()
        meta_copy(1, down(k), r, r, cross).wait_recv()
        return carry

    lax.fori_loop(1, n, take_meta, 0)
    to_smem = pltpu.make_async_copy(meta_in, meta_s, m_copy)
    to_smem.start()
    to_smem.wait()
    w_local.wait()
    w_arrives.wait_recv()

    def compute(jobs):
        for load, slot, _, state, _ in jobs:
            for j in range(CAP):
                state[0, j] = load[slot, j]
        for layer in range(layers):
            for _, slot, store, state, which in jobs:
                half = meta_s[which, slot, 0, 0]
                local = meta_s[which, slot, 0, 1]
                inner = meta_s[which, slot, 0, 2]
                for j in range(CAP):
                    other = index_ref[layer, inner + j]
                    pair = (state[layer % 2, j], state[layer % 2, other])
                    pre = jnp.dot(
                        jnp.concatenate(pair, axis=1), w_all[half, layer, local + j],
                        preferred_element_type=jnp.float32,
                    ) + bias_ref[layer, inner + j]
                    value = jnp.maximum(pre, 0.0).astype(jnp.bfloat16)
                    if layer == layers - 1:
                        store[slot, j] = value
                    else:
                        state[(layer + 1) % 2, j] = value

    def step(k, own_buf):
        slot = down(k)
        x_copy(zin, slot).wait_recv()
        compute((
            (xin, slot, fres, st_for, 1),
            (own_buf, slot, ores, st_own, 0),
        ))
        b_copy(slot).start()

    def choose(slot):
        b_copy(slot).wait_recv()
        mine = (meta_s[0, slot, 0, 3] == plane).astype(jnp.float32)
        for j in range(CAP):
            sel[slot, j] = (
                ores[slot, j].astype(jnp.float32) * mine
                + xres[slot, j].astype(jnp.float32) * (1.0 - mine)
            ).astype(jnp.bfloat16)

    def send_back(k, carry):
        slot = down(k)
        choose(slot)
        f_copy(slot, r).start()
        return carry

    forward(LAG)
    step(0, slots)

    def first(k, carry):
        forward(k + LAG)
        step(k, zin)
        return carry

    def middle(k, carry):
        forward(k + LAG)
        step(k, zin)
        return send_back(k - BACK, carry)

    def late(k, carry):
        step(k, zin)
        return send_back(k - BACK, carry)

    lax.fori_loop(1, BACK + 1, first, 0)
    choose(r)
    lax.fori_loop(BACK + 1, n - LAG, middle, 0)
    lax.fori_loop(n - LAG, n, late, 0)
    lax.fori_loop(n - BACK, n, send_back, 0)

    def take(k, carry):
        f_copy(r, down(k)).wait_recv()
        return carry

    lax.fori_loop(1, n, take, 0)
    fin[r] = sel[r]
    for p in range(live):
        out_ref[:, p * tile:(p + 1) * tile] = fin[home_ref[0, p], home_ref[1, p]]

    def drain(k, carry):
        row = up(k)
        meta_copy(0, r, row, row, g).wait_send()
        meta_copy(1, r, row, row, cross).wait_send()
        z_copy(row, r).wait_send()
        x_copy(zin, row).wait_send()
        b_copy(row).wait_send()
        f_copy(row, r).wait_send()
        return carry

    lax.fori_loop(1, n, drain, 0)
    meta_copy(1, r, r, r, cross).wait_send()
    x_copy(slots, r).wait_send()
    b_copy(r).wait_send()
    w_remote.wait_send()


def fused_shards(activations, weight_tiles, tile_index, bias_terms, demand):
    n = lax.axis_size("rows")
    layers, held, kinds, tile, _ = weight_tiles.shape
    per_range = held * lax.axis_size("grp")
    depth = activations.shape[0]
    blocks = demand[0]
    owners, within, member = blocks // per_range, blocks % per_range, blocks % CAP
    placing = (owners[None, None, :] == jnp.arange(n, dtype=jnp.int32)[:, None, None]) & (
        member[None, None, :] == jnp.arange(CAP, dtype=jnp.int32)[None, :, None]
    )
    places = jnp.arange(blocks.shape[0], dtype=jnp.int32)
    pos = jnp.sum(jnp.where(placing, places, 0), axis=2)
    starts = jnp.sum(jnp.where(placing[:, 0], within, 0), axis=1)
    chip_blocks = held * CORES
    inner = starts % chip_blocks
    facts = jnp.stack([inner // held, inner % held, inner, starts // chip_blocks], axis=1)
    meta = jnp.pad(facts, ((0, 0), (0, 124)))[:, None, :]
    home = jnp.stack([owners, member])
    chip = (lax.axis_index("rows") * PLANES + lax.axis_index("grp") // CORES) * chip_blocks
    others = lax.dynamic_slice_in_dim(tile_index[:, :, 0], chip, chip_blocks, axis=1) % CAP
    bias = lax.dynamic_slice_in_dim(bias_terms, chip * tile, chip_blocks * tile, axis=1)
    bias = bias.reshape(layers, chip_blocks, 1, tile)
    weights = weight_tiles.reshape(layers, held, kinds * tile, tile)
    columns = activations.reshape(depth, blocks.shape[0], tile).transpose(1, 0, 2)
    smem = pl.BlockSpec(memory_space=pltpu.SMEM)
    vmem = pl.BlockSpec(memory_space=pltpu.VMEM)
    slot = pltpu.VMEM((n, CAP, depth, tile), jnp.bfloat16)
    sems = pltpu.SemaphoreType.DMA((n,))
    return pl.pallas_call(
        functools.partial(fused_kernel, n),
        out_shape=jax.ShapeDtypeStruct(activations.shape, jnp.bfloat16),
        in_specs=[smem, smem, smem, vmem, vmem, vmem, pl.BlockSpec(memory_space=pl.ANY)],
        out_specs=vmem,
        scratch_shapes=[
            pltpu.VMEM((CORES, layers, held, kinds * tile, tile), jnp.bfloat16),
            slot, slot, slot, slot, slot, slot, slot, slot,
            pltpu.VMEM((2, CAP, depth, tile), jnp.bfloat16),
            pltpu.VMEM((2, CAP, depth, tile), jnp.bfloat16),
            pltpu.VMEM((2, n, 1, 128), jnp.int32),
            pltpu.SMEM((2, n, 1, 128), jnp.int32),
            pltpu.SemaphoreType.DMA((3,)),
            pltpu.SemaphoreType.DMA((2, n)),
            pltpu.SemaphoreType.DMA((2, n)),
            pltpu.SemaphoreType.DMA,
            sems, sems, sems, sems, sems, sems, sems, sems,
        ],
        compiler_params=pltpu.CompilerParams(
            collective_id=0, has_side_effects=True, vmem_limit_bytes=40 * 1024 * 1024
        ),
    )(pos, home, others, meta, columns, bias, weights)


def solution(mesh):
    def shards(activations, weight_tiles, tile_index, bias_terms, demand):
        whole_groups = weight_tiles.shape[1] % CAP == 0 and weight_tiles.shape[2] == 2
        if whole_groups and mesh.shape["grp"] == PLANES * CORES and mesh.shape["rows"] > LAG + BACK:
            return fused_shards(activations, weight_tiles, tile_index, bias_terms, demand)
        return gathered_shards(activations, weight_tiles, tile_index, bias_terms, demand)

    return jax.shard_map(
        shards,
        mesh=mesh,
        in_specs=(
            P(("rows", "grp"), None),
            P(None, ("rows", "grp"), None, None, None),
            P(),
            P(),
            P(("rows", "grp"), None),
        ),
        out_specs=P(("rows", "grp"), None),
        check_vma=False,
    )
```
